256 devices in a mesh: level: 32 (over z, y), bal: 8 (over x, core).
Axes of the slice: x: 4, y: 4, z: 8, core: 2. Of those that a mesh axis runs over, the one named last changes fastest.
Arguments:
- patches: float32 [6144, 5, 4096], P(('level', 'bal')), may hold values from -6 to 6
- patch_ids: int32 [6144], P(('level', 'bal')), may hold values from 0 to 6143, each once
- live: int32 [256], P(('level', 'bal')), may hold values from 4 to 12, as said below
- counts: int32 [3, 256], P(None, ('level', 'bal')), may hold values from 0 to 4, as said below
- parent_of: int32 [6144], replicated, may hold values from 0 to 63
Outputs:
- new_patches: float32 [6144, 5, 4096], P(('level', 'bal'))
- new_ids: int32 [6144], P(('level', 'bal'))
- coarse: float32 [64, 5, 512], P('level')
The draws below stay inside these ranges and needn't reach their ends.
Inputs may be any that keep to these rules, and one draw needn't show every extreme that they name: In every level group one device holds exactly 12 live patches. counts[r, d] never exceeds the live patches of device d at the start of round r; in every round and level group some device sends exactly 4.
All inputs are finite; a program needn't handle non-finite values.
Results may differ from the reference program's by a relative error of at most 0.0003.
Values sent between devices are 32-bit elements; how exact they have to be, the bound alone decides.
No kernel may reach another device: no remote copies, remote signals or barrier semaphores. Data moves between devices by JAX's collectives and lax.ppermute only.
A program may use at most 64 MiB of HBM per device.

```python
import jax
import jax.numpy as jnp
import numpy as np

EDGE = 16
VARS = 5
SEND_MOST = 4
LOAD_MOST = 12
ROUNDS = 3
GROUP = 8
LEVELS = 32
CAP = 24
SLOTS = 6144
CELLS = 4096
COARSE = 512
PARENTS = 64


def plan_layout(key):
    first_key = jax.random.fold_in(key, 11)
    second_key = jax.random.fold_in(key, 12)
    third_key = jax.random.fold_in(key, 13)
    members = jnp.arange(GROUP, dtype=jnp.int32)
    loads = jax.random.randint(first_key, (LEVELS, GROUP), SEND_MOST, LOAD_MOST + 1)
    heavy = jax.random.randint(second_key, (LEVELS,), 0, GROUP)
    light = (heavy + 1 + jax.random.randint(third_key, (LEVELS,), 0, GROUP - 1)) % GROUP
    loads = jnp.where(members[None, :] == heavy[:, None], LOAD_MOST, loads)
    loads = jnp.where(members[None, :] == light[:, None], SEND_MOST, loads)
    held_count = loads
    sends = []
    for turn_index in range(ROUNDS):
        turn_key = jax.random.fold_in(key, 100 + turn_index)
        limit = jnp.minimum(SEND_MOST, held_count)
        drawn = jax.random.randint(turn_key, (LEVELS, GROUP), SEND_MOST // 2, SEND_MOST + 1)
        sent_count = jnp.minimum(drawn, limit)
        breaker = jax.random.permutation(jax.random.fold_in(turn_key, 7), GROUP).astype(jnp.int32)
        score = held_count * GROUP + breaker[None, :]
        busiest = jnp.argmax(score, axis=1).astype(jnp.int32)
        sent_count = jnp.where(members[None, :] == busiest[:, None], limit, sent_count)
        partner = members ^ 1 << turn_index
        held_count = held_count - sent_count + sent_count[:, partner]
        sends.append(sent_count)
    return (loads.reshape(LEVELS * GROUP), jnp.stack(sends).reshape(ROUNDS, LEVELS * GROUP))


def draw_live(key, part):
    return plan_layout(key)[0].astype(jnp.int32)


def draw_counts(key, part):
    return plan_layout(key)[1].astype(jnp.int32)


def place_ends(values, own_key, smallest, largest):
    longest = values.shape.index(max(values.shape))
    spots = []
    for shift in (0, 1):
        where = [jax.random.randint(jax.random.fold_in(own_key, axis), (), 0, length) for axis, length in enumerate(values.shape)]
        where[longest] = (where[longest] + shift) % values.shape[longest]
        spots.append(tuple(where))
    return values.at[spots[0]].set(smallest).at[spots[1]].set(largest)


def level_of(stream_key, shape, pieces, low, high):
    def one(position, shards_of):
        draws = jax.random.uniform(jax.random.fold_in(jax.random.fold_in(stream_key, 6), position), (shards_of,), jnp.float32, low / len(pieces), high / len(pieces))
        return jnp.repeat(jnp.exp(draws), shape[position] // shards_of).reshape((-1,) + (1,) * (len(shape) - position - 1))

    loudness = one(*pieces[0])
    for cut in pieces[1:]:
        loudness = loudness * one(*cut)
    return loudness


def bell_draw(rng, dims, width, most, split=(), held_as=jnp.bfloat16):
    values = width * jax.random.normal(rng, dims, jnp.float32)
    if split:
        values = values * level_of(rng, dims, split, -0.22, 0.18)
    return jnp.clip(values, -most, most).astype(held_as)


def setup_inputs(seed: int = 0) -> dict:
    splits = jax.random.split(jax.random.key(seed), 6)
    patches = bell_draw(splits[0], (SLOTS, VARS, CELLS), 1.0, 6.0, ((0, 256),), jnp.float32)
    patch_ids = jax.random.permutation(splits[1], SLOTS).astype(jnp.int32)
    live = draw_live(jax.random.fold_in(splits[5], 71), 0)
    counts = draw_counts(jax.random.fold_in(splits[5], 71), 0)
    parent_of = place_ends(jax.random.randint(splits[4], (SLOTS,), 0, PARENTS), jax.random.fold_in(splits[4], 1), 0, PARENTS - 1).astype(jnp.int32)
    return {"patches": patches, "patch_ids": patch_ids, "live": live, "counts": counts, "parent_of": parent_of}


def restrict(fine_rows):
    leading = fine_rows.shape[:-1]
    half_edge = EDGE // 2
    blocks = fine_rows.reshape(leading + (half_edge, 2, half_edge, 2, half_edge, 2))
    return jnp.mean(blocks, axis=(-5, -3, -1)).reshape(leading + (half_edge * half_edge * half_edge,))


def take_top(fine_rows, fine_ids, held_count, sent_count):
    capacity = fine_rows.shape[0]
    lane_index = jnp.arange(SEND_MOST, dtype=jnp.int32)
    pick_index = jnp.clip(held_count - sent_count + lane_index, 0, capacity - 1)
    is_valid = lane_index < sent_count
    return (jnp.where(is_valid[:, None, None], fine_rows[pick_index], 0.0),
            jnp.where(is_valid, fine_ids[pick_index], -1))


def place_rows(fine_rows, fine_ids, kept_count, in_rows, in_ids):
    capacity = fine_rows.shape[0]
    slot_index = jnp.arange(capacity, dtype=jnp.int32)
    offset = slot_index - kept_count
    is_hit = (offset >= 0) & (offset < SEND_MOST)
    place_index = jnp.clip(offset, 0, SEND_MOST - 1)
    is_kept = slot_index < kept_count
    new_rows = jnp.where(is_kept[:, None, None], fine_rows,
                         jnp.where(is_hit[:, None, None], in_rows[place_index], 0.0))
    new_ids = jnp.where(is_kept, fine_ids, jnp.where(is_hit, in_ids[place_index], -1))
    return new_rows, new_ids


def reference(patches, patch_ids, live, counts, parent_of):
    devices = LEVELS * GROUP
    grid_rows = patches.reshape(devices, CAP, VARS, CELLS)
    grid_ids = patch_ids.reshape(devices, CAP)
    slot_index = jnp.arange(CAP, dtype=jnp.int32)
    held_count = live
    is_kept = slot_index[None, :] < held_count[:, None]
    grid_rows = jnp.where(is_kept[:, :, None, None], grid_rows, 0.0)
    grid_ids = jnp.where(is_kept, grid_ids, -1)
    members = np.arange(devices)
    for turn_index in range(ROUNDS):
        partner = (members // GROUP) * GROUP + ((members % GROUP) ^ (1 << turn_index))
        sent_count = counts[turn_index]
        out_rows, out_ids = jax.vmap(take_top)(grid_rows, grid_ids, held_count, sent_count)
        kept_count = held_count - sent_count
        grid_rows, grid_ids = jax.vmap(place_rows)(grid_rows, grid_ids, kept_count, out_rows[partner], out_ids[partner])
        held_count = kept_count + sent_count[partner]
    reduced = restrict(grid_rows).reshape(devices * CAP, VARS * COARSE)
    flat_ids = grid_ids.reshape(-1)
    parent = jnp.where(flat_ids >= 0, parent_of[jnp.clip(flat_ids, 0, SLOTS - 1)], PARENTS).astype(jnp.int32)
    coarse = jax.ops.segment_sum(reduced, parent, num_segments=PARENTS + 1)[:PARENTS]
    return grid_rows.reshape(SLOTS, VARS, CELLS), flat_ids, coarse.reshape(PARENTS, VARS, COARSE)
```

```python
import functools

import jax
import jax.numpy as jnp
from jax import lax
from jax.experimental import pallas as pl
from jax.experimental.pallas import tpu as pltpu
from jax.sharding import PartitionSpec as P

VARS = 5
SEND = 4
TILE = 8
TILES = 3
LIVE_TILES = 2
LIVE = 12
LANES = 128
SPAN = 32
ROWS = VARS * SPAN
TILE_ROWS = ROWS * TILE
HEAD = SEND * ROWS
MSG = HEAD + 8
FINE = 20
PAR_DEV = 2
F32 = jnp.float32
I32 = jnp.int32

SMEM = pl.BlockSpec(memory_space=pltpu.SMEM)
VMEM = pl.BlockSpec(memory_space=pltpu.VMEM)
ANY = pl.BlockSpec(memory_space=pl.ANY)


def from_partner(array, mask):
    return lax.ppermute(array, "bal", [(i, i ^ mask) for i in range(8)])


def lanes():
    return lax.broadcasted_iota(I32, (8, LANES), 1)


def row_of(slot):
    return (slot // TILE) * TILE_ROWS + slot % TILE


def move(dst, dst_row, dst_step, src, src_row, src_step):
    def at(ref, row, step, chunk):
        start = row + chunk * 8 * step
        if step == 1:
            return pl.ds(pl.multiple_of(start, 8), 8)
        return pl.ds(start, 8, stride=step)

    for chunk in range(ROWS // 8):
        dst[at(dst, dst_row, dst_step, chunk), :] = src[at(src, src_row, src_step, chunk), :]


def load_kernel(live, counts, ids, x, held, msg, sems):
    copies = []
    for tile in range(LIVE_TILES):
        for var in range(VARS):
            part = pl.ds((tile * VARS + var) * SPAN * TILE, SPAN * TILE)
            copies.append(pltpu.make_async_copy(x.at[var, tile], held.at[part, :], sems.at[tile * VARS + var]))
    for copy in copies:
        copy.start()
    sent = counts[0, 0]
    first = live[0] - sent
    lane = lanes()
    head = jnp.where(lane == SEND, sent.astype(F32), 0.0)
    for lane_id in range(SEND):
        slot = jnp.minimum(first + lane_id, LIVE - 1)
        head = jnp.where(lane == lane_id, ids[slot].astype(F32), head)
    msg[pl.ds(HEAD, 8), :] = head
    for copy in copies:
        copy.wait()
    for piece in range(SEND):

        @pl.when(piece < sent)
        def _():
            move(msg, piece * ROWS, 1, held, row_of(first + piece), TILE)


def restrict_kernel(live, ids, held, parent_of, weight, out, fine, parents, sem):
    table = pltpu.make_async_copy(parent_of, parents, sem)
    table.start()
    groups = LIVE_TILES * VARS * SPAN // 8
    x = held[...].reshape(groups, 8, TILE, LANES)
    pieces = []
    for half in range(2):
        for side in range(2):
            pieces.append((x[:, half * 4 + side] + x[:, half * 4 + side + 2]).reshape(groups * TILE, LANES))
    pairs = jnp.concatenate(pieces, axis=1)
    high = pairs.astype(jnp.bfloat16)
    low = (pairs - high.astype(F32)).astype(jnp.bfloat16)
    w = weight[...]
    fine[...] = jnp.dot(high, w, preferred_element_type=F32) + jnp.dot(low, w, preferred_element_type=F32)
    out[...] = jnp.zeros_like(out)
    table.wait()
    for slot in range(LIVE):

        @pl.when(slot < live[0])
        def _():
            parent = parents[ids[slot]]
            base = (parent // PAR_DEV) * (FINE * PAR_DEV) + parent % PAR_DEV
            src = (slot // TILE) * (FINE * TILE) + slot % TILE
            for start, size in ((0, 8), (8, 8), (16, 4)):
                to = pl.ds(base + start * PAR_DEV, size, stride=PAR_DEV)
                out[to, :] += fine[pl.ds(src + start * TILE, size, stride=TILE), :]


def number(ref, lane):
    return ref[HEAD, lane].astype(I32)


def merged_ids(own, came, kept, lane):
    return jnp.where(lane < kept, own, pltpu.roll(came, kept, 1))


def pick_kernel(live, counts, ids, held, came, last, below):
    lane = lanes()
    kept = live[0] - counts[0, 0]
    held_count = kept + number(came, SEND)
    sent = counts[1, 0]
    ids_now = merged_ids(ids[...], came[pl.ds(HEAD, 8), :], kept, lane)
    for msg, first, low, high in (
        (last, held_count - sent, 0, sent),
        (below, held_count - sent - SEND, 0, SEND),
    ):
        head = pltpu.roll(ids_now, lax.rem(LANES - first, LANES), 1)
        head = jnp.where(lane == SEND, sent.astype(F32), head)
        head = jnp.where(lane == SEND + 1, counts[2, 0].astype(F32), head)
        msg[pl.ds(HEAD, 8), :] = head
        for piece in range(SEND):
            slot = first + piece
            used = jnp.logical_and(slot >= 0, piece < high)

            @pl.when(jnp.logical_and(used, slot < kept))
            def _():
                move(msg, piece * ROWS, 1, held, row_of(slot), TILE)

            @pl.when(jnp.logical_and(used, slot >= kept))
            def _():
                move(msg, piece * ROWS, 1, came, (slot - kept) * ROWS, 1)


def place_kernel(live, counts, ids, held, came, near, far, cross, out, new_ids, full, sems):
    lane = lanes()
    kept = live[0] - counts[0, 0]
    c0 = number(came, SEND)
    c1, c2 = counts[1, 0], counts[2, 0]
    n1 = number(near, SEND)
    f2 = number(far, SEND + 1)
    x1 = number(cross, SEND)
    own = kept + c0 - c1 - jnp.maximum(c2 - n1, 0)
    from_near = jnp.maximum(n1 - c2, 0)
    from_far = jnp.maximum(f2 - x1, 0)
    from_cross = jnp.minimum(x1, f2)
    bare = jnp.minimum(own, kept)

    sub = lax.broadcasted_iota(I32, (TILE, LANES), 0)
    for tile in range(TILES):
        rows = pl.ds(tile * TILE_ROWS, TILE_ROWS)
        if tile < LIVE_TILES:
            keep = (sub + tile * TILE < bare)[None]
            part = held[rows, :].reshape(ROWS, TILE, LANES)
            full[rows, :] = jnp.where(keep, part, 0.0).reshape(TILE_ROWS, LANES)
        else:
            full[rows, :] = jnp.zeros((TILE_ROWS, LANES), F32)

    marks = ids[...]
    at = kept
    new = jnp.where(lane < bare, marks, -1.0)
    start = bare
    for msg, skip, amount in (
        (came, 0, own - bare),
        (near, 0, from_near),
        (far, SEND - from_far, from_far),
        (cross, x1 - from_cross, from_cross),
    ):
        shift = lax.rem(start - skip + LANES, LANES)
        moved = pltpu.roll(msg[pl.ds(HEAD, 8), :], shift, 1)
        inside = jnp.logical_and(lane >= start, lane < start + amount)
        new = jnp.where(inside, moved, new)
        for piece in range(SEND):

            @pl.when(piece < amount)
            def _(msg=msg, piece=piece, start=start, skip=skip):
                move(full, row_of(start + piece), TILE, msg, (skip + piece) * ROWS, 1)

        start = start + amount
    new_ids[...] = new.astype(I32)
    copies = []
    for tile in range(TILES):
        for var in range(VARS):
            part = pl.ds((tile * VARS + var) * SPAN * TILE, SPAN * TILE)
            copies.append(pltpu.make_async_copy(full.at[part, :], out.at[var, tile], sems.at[tile * VARS + var]))
    for copy in copies:
        copy.start()
    for copy in copies:
        copy.wait()


def restriction_weight():
    lane = jnp.arange(LANES)
    column = ((lane // 32) * 8 + (lane % 16) // 2)[:, None]
    target = jnp.arange(LANES)[None, :]
    return jnp.concatenate(
        [jnp.where(target == group * 32 + column, 0.125, 0.0) for group in range(4)], axis=0
    ).astype(jnp.bfloat16)


def call(kernel, outs, ins, out_specs, scratch=(), **kw):
    return pl.pallas_call(
        kernel, out_shape=outs, in_specs=ins, out_specs=out_specs, scratch_shapes=list(scratch), **kw
    )


def per_device(patches, patch_ids, live, counts, parent_of):
    slots = patches.shape[0]
    levels = lax.axis_size("level")
    x = patches.transpose(1, 0, 2).reshape(VARS, TILES, TILE, SPAN, LANES)
    x = x.transpose(0, 1, 3, 2, 4).reshape(VARS, TILES, SPAN * TILE, LANES)
    marks = jnp.broadcast_to(jnp.pad(patch_ids.astype(F32), (0, LANES - slots))[None], (8, LANES))
    message = jax.ShapeDtypeStruct((MSG, LANES), F32)
    held, first = call(
        load_kernel,
        (jax.ShapeDtypeStruct((LIVE_TILES * TILE_ROWS, LANES), F32), message),
        [SMEM, SMEM, SMEM, ANY],
        (VMEM, VMEM),
        [pltpu.SemaphoreType.DMA((LIVE_TILES * VARS,))],
        name="load",
    )(live, counts, patch_ids, x)
    came = from_partner(first, 1)
    block = FINE * PAR_DEV
    partial = call(
        restrict_kernel,
        jax.ShapeDtypeStruct((levels * block, LANES), F32),
        [SMEM, SMEM, VMEM, ANY, VMEM],
        VMEM,
        [
            pltpu.VMEM((LIVE_TILES * TILE * FINE, LANES), F32),
            pltpu.SMEM(parent_of.shape, I32),
            pltpu.SemaphoreType.DMA,
        ],
        name="restrict",
    )(live, patch_ids, held, parent_of, restriction_weight())
    last, below = call(
        pick_kernel, (message, message), [SMEM, SMEM, VMEM, VMEM, VMEM], (VMEM, VMEM), name="pick"
    )(live, counts, marks, held, came)
    far = from_partner(below, 4)
    near = from_partner(last, 2)
    cross = from_partner(last, 6)

    tiles = lax.all_to_all(partial.reshape(levels, block, LANES), "level", 0, 0, tiled=True)
    sums = jnp.sum(tiles, axis=0)
    sums = sums + from_partner(sums, 2) + from_partner(sums, 6) + from_partner(sums, 4)
    sums = sums + from_partner(sums, 1)
    coarse = sums.reshape(VARS, FINE // VARS, PAR_DEV, LANES).transpose(2, 0, 1, 3).reshape(PAR_DEV, VARS, -1)

    out, new_ids = call(
        place_kernel,
        (jax.ShapeDtypeStruct((VARS, TILES, SPAN * TILE, LANES), F32), jax.ShapeDtypeStruct((8, LANES), I32)),
        [SMEM, SMEM, VMEM, VMEM, VMEM, VMEM, VMEM, VMEM],
        (ANY, VMEM),
        [pltpu.VMEM((TILES * TILE_ROWS, LANES), F32), pltpu.SemaphoreType.DMA((TILES * VARS,))],
        name="place",
    )(live, counts, marks, held, came, near, far, cross)
    out = out.reshape(VARS, TILES, SPAN, TILE, LANES).transpose(0, 1, 3, 2, 4)
    out = out.reshape(VARS, slots, SPAN * LANES).transpose(1, 0, 2)
    return (out, new_ids[0, :slots], coarse)


def solution(mesh):
    return jax.shard_map(
        per_device,
        mesh=mesh,
        in_specs=(
            P(("level", "bal"), None, None),
            P(("level", "bal")),
            P(("level", "bal")),
            P(None, ("level", "bal")),
            P(),
        ),
        out_specs=(P(("level", "bal"), None, None), P(("level", "bal")), P("level", None, None)),
        check_vma=False,
    )
```

```python
import jax
import jax.numpy as jnp
from jax import lax
from jax.experimental import pallas as pl
from jax.experimental.pallas import tpu as pltpu
from jax.sharding import PartitionSpec as P


VARS = 5
SEND = 4
TILE = 8
TILES = 3
LIVE_TILES = 2
LIVE = 12
LANES = 128
SPAN = 32
ROWS = VARS * SPAN
TILE_ROWS = ROWS * TILE
HEAD = SEND * ROWS
MSG = HEAD + 8
FINE = 20
PAR_DEV = 2
NEAR_LEVELS = 4
FAR_LEVELS = 8
PIECE = FAR_LEVELS * FINE
F32 = jnp.float32
I32 = jnp.int32
LIVE_AT = 16
COUNTS_AT = 17
PARENTS_AT = 32

SMEM = pl.BlockSpec(memory_space=pltpu.SMEM)
VMEM = pl.BlockSpec(memory_space=pltpu.VMEM)
HBM = pl.BlockSpec(memory_space=pltpu.HBM)


def from_partner(array, axis, mask):
    return lax.ppermute(array, axis, [(i, i ^ mask) for i in range(lax.axis_size(axis))])


def lanes():
    return lax.broadcasted_iota(I32, (8, LANES), 1)


def row_of(slot):
    return (slot // TILE) * TILE_ROWS + slot % TILE


def fill_weight(weight):
    lane = lax.broadcasted_iota(I32, (LANES, LANES), 0)
    target = lax.broadcasted_iota(I32, (LANES, LANES), 1)
    column = (lane // 32) * 8 + (lane % 16) // 2
    for group in range(4):
        part = jnp.where(target == group * 32 + column, 0.125, 0.0)
        weight[pl.ds(group * LANES, LANES), :] = part.astype(jnp.bfloat16)


def rows_at(row, step, chunk):
    start = row + chunk * 8 * step
    if step == 1:
        return pl.ds(pl.multiple_of(start, 8), 8)
    return pl.ds(start, 8, stride=step)


def move(dst, dst_row, dst_step, src, src_row, src_step, chunks=range(ROWS // 8)):
    for chunk in chunks:
        dst[rows_at(dst_row, dst_step, chunk), :] = src[rows_at(src_row, src_step, chunk), :]


def block_copies(hbm, vmem, sems, tiles, var, inward):
    copies = []
    for tile in tiles:
        part = vmem.at[pl.ds((tile * VARS + var) * SPAN * TILE, SPAN * TILE), :]
        ends = (hbm.at[var, tile], part) if inward else (part, hbm.at[var, tile])
        copies.append(pltpu.make_async_copy(*ends, sems.at[tile * VARS + var]))
    return copies


def load_kernel(
    live, counts, ids, parent_of, x, held, msg, weight, info, counts_s, ids_s, parents, sems, small_sems
):
    small = [
        pltpu.make_async_copy(src, dst, small_sems.at[i])
        for i, (src, dst) in enumerate(((counts, counts_s), (ids, ids_s), (parent_of, parents)))
    ]
    for copy in small:
        copy.start()
    copies = []
    for var in range(VARS):
        copies += block_copies(x, held, sems, range(LIVE_TILES), var, True)
    for copy in copies:
        copy.start()
    fill_weight(weight)
    for copy in small:
        copy.wait()
    sent = counts_s[0]
    first = live[0] - sent
    lane = lanes()
    head = jnp.where(lane == SEND, sent.astype(F32), 0.0)
    for lane_id in range(SEND):
        slot = jnp.minimum(first + lane_id, LIVE - 1)
        head = jnp.where(lane == lane_id, ids_s[slot].astype(F32), head)
    msg[pl.ds(HEAD, 8), :] = head
    numbers = jnp.where(lane == LIVE_AT, live[0], 0)
    for turn in range(3):
        numbers = jnp.where(lane == COUNTS_AT + turn, counts_s[turn], numbers)
    for slot in range(LIVE):
        mark = ids_s[slot]
        numbers = jnp.where(lane == slot, mark, numbers)
        numbers = jnp.where(lane == PARENTS_AT + slot, parents[mark], numbers)
    info[...] = numbers
    for copy in copies:
        copy.wait()
    for piece in range(SEND):

        @pl.when(piece < sent)
        def _(piece=piece):
            move(msg, piece * ROWS, 1, held, row_of(first + piece), TILE)


def restrict_kernel(info, held, weight, mine, other, fine):
    groups = LIVE_TILES * VARS * SPAN // 8
    x = held[...].reshape(groups, 8, TILE, LANES)
    pieces = []
    for half in range(2):
        for side in range(2):
            pieces.append((x[:, half * 4 + side] + x[:, half * 4 + side + 2]).reshape(groups * TILE, LANES))
    pairs = jnp.concatenate(pieces, axis=1)
    high = pairs.astype(jnp.bfloat16)
    low = (pairs - high.astype(F32)).astype(jnp.bfloat16)
    w = weight[...]
    fine[...] = jnp.dot(high, w, preferred_element_type=F32) + jnp.dot(low, w, preferred_element_type=F32)
    mine[...] = jnp.zeros_like(mine)
    other[...] = jnp.zeros_like(other)
    core = lax.axis_index("bal") % PAR_DEV
    place = lax.axis_index("level") % NEAR_LEVELS
    live = info[0, LIVE_AT]
    for slot in range(LIVE):
        parent = info[0, PARENTS_AT + slot]
        level = parent // PAR_DEV
        near = jnp.bitwise_xor(level % NEAR_LEVELS, place)
        base = near * PIECE + (level // NEAR_LEVELS) * FINE
        src = (slot // TILE) * (FINE * TILE) + slot % TILE
        here = parent % PAR_DEV == core
        for out, wanted in ((mine, here), (other, jnp.logical_not(here))):

            @pl.when(jnp.logical_and(slot < live, wanted))
            def _(out=out, base=base, src=src):
                for start, size in ((0, 8), (8, 8), (16, 4)):
                    out[pl.ds(base + start, size), :] += fine[pl.ds(src + start * TILE, size, stride=TILE), :]


def add_kernel(mine, other, *outs):
    for near, out in enumerate(outs):
        rows = pl.ds(near * PIECE, PIECE)
        out[...] = mine[rows, :] + other[rows, :]


def number(ref, lane):
    return ref[HEAD, lane].astype(I32)


def head_of(ref):
    return ref[pl.ds(HEAD, 8), :]


def pick_kernel(info, held, came, last, below):
    lane = lanes()
    sent = info[0, COUNTS_AT + 1]
    kept = info[0, LIVE_AT] - info[0, COUNTS_AT]
    held_count = kept + number(came, SEND)
    marks = info[...].astype(F32)
    marks = jnp.where(lane < kept, marks, pltpu.roll(head_of(came), kept, 1))
    for msg, first, pieces in ((last, held_count - sent, sent), (below, held_count - sent - SEND, SEND)):
        head = pltpu.roll(marks, lax.rem(LANES - first, LANES), 1)
        head = jnp.where(lane == SEND, sent.astype(F32), head)
        head = jnp.where(lane == SEND + 1, info[0, COUNTS_AT + 2].astype(F32), head)
        msg[pl.ds(HEAD, 8), :] = head
        for piece in range(SEND):
            slot = first + piece
            used = jnp.logical_and(slot >= 0, piece < pieces)

            @pl.when(jnp.logical_and(used, slot < kept))
            def _(msg=msg, piece=piece, slot=slot):
                move(msg, piece * ROWS, 1, held, row_of(slot), TILE)

            @pl.when(jnp.logical_and(used, slot >= kept))
            def _(msg=msg, piece=piece, slot=slot):
                move(msg, piece * ROWS, 1, came, (slot - kept) * ROWS, 1)


def place_kernel(info, x, came, near, far, cross, out, new_ids, full, in_sems, out_sems):
    loads = []
    for var in range(VARS):
        loads.append(block_copies(x, full, in_sems, range(LIVE_TILES), var, True))
    for copies in loads:
        for copy in copies:
            copy.start()
    lane = lanes()
    kept = info[0, LIVE_AT] - info[0, COUNTS_AT]
    c0 = number(came, SEND)
    c1, c2 = info[0, COUNTS_AT + 1], info[0, COUNTS_AT + 2]
    n1 = number(near, SEND)
    f2 = number(far, SEND + 1)
    x1 = number(cross, SEND)
    own = kept + c0 - c1 - jnp.maximum(c2 - n1, 0)
    from_near = jnp.maximum(n1 - c2, 0)
    from_far = jnp.maximum(f2 - x1, 0)
    from_cross = jnp.minimum(x1, f2)
    bare = jnp.minimum(own, kept)

    new = jnp.where(lane < bare, info[...].astype(F32), -1.0)
    start = bare
    parts = []
    for msg, skip, amount in (
        (came, 0, own - bare),
        (near, 0, from_near),
        (far, SEND - from_far, from_far),
        (cross, x1 - from_cross, from_cross),
    ):
        moved = pltpu.roll(head_of(msg), lax.rem(start - skip + LANES, LANES), 1)
        new = jnp.where(jnp.logical_and(lane >= start, lane < start + amount), moved, new)
        parts.append((msg, skip, amount, start))
        start = start + amount
    new_ids[...] = new[0:1, : TILE * TILES].astype(I32)

    sub = lax.broadcasted_iota(I32, (TILE, LANES), 0)
    stores = []
    for var in range(VARS):
        for copy in loads[var]:
            copy.wait()
        for tile in range(TILES):
            rows = pl.ds((tile * VARS + var) * SPAN * TILE, SPAN * TILE)
            if tile < LIVE_TILES:
                keep = (sub + tile * TILE < bare)[None]
                part = full[rows, :].reshape(SPAN, TILE, LANES)
                full[rows, :] = jnp.where(keep, part, 0.0).reshape(SPAN * TILE, LANES)
            else:
                full[rows, :] = jnp.zeros((SPAN * TILE, LANES), F32)
        chunks = range(var * SPAN // 8, (var + 1) * SPAN // 8)
        for msg, skip, amount, start in parts:
            for piece in range(SEND):

                @pl.when(piece < amount)
                def _(msg=msg, piece=piece, start=start, skip=skip, chunks=chunks):
                    move(full, row_of(start + piece), TILE, msg, (skip + piece) * ROWS, 1, chunks)

        stores += block_copies(out, full, out_sems, range(TILES), var, False)
        for copy in stores[-TILES:]:
            copy.start()
    for copy in stores:
        copy.wait()


def final_kernel(mine, other, out):
    core = lax.axis_index("bal") % PAR_DEV
    out[pl.ds(core, FINE, stride=PAR_DEV), :] = mine[...]
    out[pl.ds(1 - core, FINE, stride=PAR_DEV), :] = other[...]


def call(kernel, outs, in_specs, args, out_specs, scratch=()):
    args = [
        pltpu.with_memory_space_constraint(arg, spec.memory_space) if spec in (VMEM, HBM) else arg
        for arg, spec in zip(args, in_specs, strict=True)
    ]
    kernel = pl.pallas_call(
        kernel,
        out_shape=outs,
        in_specs=in_specs,
        out_specs=out_specs,
        scratch_shapes=list(scratch),
        compiler_params=pltpu.CompilerParams(vmem_limit_bytes=12 << 20),
    )
    return kernel(*args)


def per_device(patches, patch_ids, live, counts, parent_of):
    slots = patches.shape[0]
    x = patches.transpose(1, 0, 2).reshape(VARS, TILES, TILE, SPAN, LANES)
    x = x.transpose(0, 1, 3, 2, 4).reshape(VARS, TILES, SPAN * TILE, LANES)
    counts = counts.reshape(-1)
    message = pltpu.VMEM((MSG, LANES), F32)
    dma = pltpu.SemaphoreType.DMA
    held, first, weight, info = call(
        load_kernel,
        (
            pltpu.VMEM((LIVE_TILES * TILE_ROWS, LANES), F32),
            message,
            pltpu.VMEM((4 * LANES, LANES), jnp.bfloat16),
            pltpu.VMEM((8, LANES), I32),
        ),
        [SMEM] + [HBM] * 4,
        (live, counts, patch_ids, parent_of, x),
        (VMEM,) * 4,
        [pltpu.SMEM(a.shape, I32) for a in (counts, patch_ids, parent_of)]
        + [dma((LIVE_TILES * VARS,)), dma((3,))],
    )
    came = from_partner(first, "bal", 1)
    half = pltpu.VMEM((NEAR_LEVELS * PIECE, LANES), F32)
    mine, other = call(
        restrict_kernel,
        (half, half),
        [VMEM] * 3,
        (info, held, weight),
        (VMEM, VMEM),
        [pltpu.VMEM((LIVE_TILES * TILE * FINE, LANES), F32)],
    )
    last, below = call(pick_kernel, (message, message), [VMEM] * 3, (info, held, came), (VMEM, VMEM))
    piece = pltpu.VMEM((PIECE, LANES), F32)
    pieces = call(
        add_kernel, (piece,) * NEAR_LEVELS, [VMEM, VMEM], (mine, from_partner(other, "bal", 1)), (VMEM,) * NEAR_LEVELS
    )
    partial = pieces[0]
    for mask in range(1, NEAR_LEVELS):
        partial = partial + from_partner(pieces[mask], "level", mask)
    far = from_partner(below, "bal", 4)
    near = from_partner(last, "bal", 2)
    cross = from_partner(last, "bal", 6)

    groups = [[z * NEAR_LEVELS + y for z in range(FAR_LEVELS)] for y in range(NEAR_LEVELS)]
    tiles = lax.all_to_all(
        partial.reshape(FAR_LEVELS, FINE // 4, 4, LANES), "level", 0, 0, axis_index_groups=groups, tiled=True
    )
    sums = jnp.sum(tiles, axis=0)
    sums = sums + from_partner(sums, "bal", 2) + from_partner(sums, "bal", 6) + from_partner(sums, "bal", 4)
    sums = sums.reshape(FINE, LANES)
    coarse = call(
        final_kernel,
        jax.ShapeDtypeStruct((FINE * PAR_DEV, LANES), F32),
        [VMEM, VMEM],
        (sums, from_partner(sums, "bal", 1)),
        VMEM,
    )
    coarse = coarse.reshape(VARS, FINE // VARS, PAR_DEV, LANES).transpose(2, 0, 1, 3).reshape(PAR_DEV, VARS, -1)

    out, new_ids = call(
        place_kernel,
        (jax.ShapeDtypeStruct((VARS, TILES, SPAN * TILE, LANES), F32), jax.ShapeDtypeStruct((1, slots), I32)),
        [VMEM, HBM, VMEM, VMEM, VMEM, VMEM],
        (info, x, came, near, far, cross),
        (HBM, VMEM),
        [pltpu.VMEM((TILES * TILE_ROWS, LANES), F32), dma((LIVE_TILES * VARS,)), dma((TILES * VARS,))],
    )
    out = out.reshape(VARS, TILES, SPAN, TILE, LANES).transpose(0, 1, 3, 2, 4)
    out = out.reshape(VARS, slots, SPAN * LANES).transpose(1, 0, 2)
    return (out, new_ids.reshape(slots), coarse)


def solution(mesh):
    return jax.shard_map(
        per_device,
        mesh=mesh,
        in_specs=(
            P(("level", "bal"), None, None),
            P(("level", "bal")),
            P(("level", "bal")),
            P(None, ("level", "bal")),
            P(),
        ),
        out_specs=(P(("level", "bal"), None, None), P(("level", "bal")), P("level", None, None)),
        check_vma=False,
    )
```

```python
import jax
import jax.numpy as jnp
from jax import lax
from jax.experimental import pallas as pl
from jax.experimental.pallas import tpu as pltpu
from jax.sharding import PartitionSpec as P


VARS = 5
SEND = 4
TILE = 8
TILES = 3
LIVE_TILES = 2
LIVE = 12
LANES = 128
SPAN = 32
ROWS = VARS * SPAN
TILE_ROWS = ROWS * TILE
HEAD = SEND * ROWS
MSG = HEAD + 8
FINE = 20
PAR_DEV = 2
F32 = jnp.float32
I32 = jnp.int32
LIVE_AT = 16
COUNTS_AT = 17

SMEM = pl.BlockSpec(memory_space=pltpu.SMEM)
VMEM = pl.BlockSpec(memory_space=pltpu.VMEM)
HBM = pl.BlockSpec(memory_space=pltpu.HBM)


def from_partner(array, axis, mask):
    return lax.ppermute(array, axis, [(i, i ^ mask) for i in range(lax.axis_size(axis))])


def lanes():
    return lax.broadcasted_iota(I32, (8, LANES), 1)


def row_of(slot):
    return (slot // TILE) * TILE_ROWS + slot % TILE


def fill_weight(weight):
    lane = lax.broadcasted_iota(I32, (LANES, LANES), 0)
    target = lax.broadcasted_iota(I32, (LANES, LANES), 1)
    column = (lane // 32) * 8 + (lane % 16) // 2
    for group in range(4):
        part = jnp.where(target == group * 32 + column, 0.125, 0.0)
        weight[pl.ds(group * LANES, LANES), :] = part.astype(jnp.bfloat16)


def rows_at(row, step, chunk):
    start = row + chunk * 8 * step
    if step == 1:
        return pl.ds(pl.multiple_of(start, 8), 8)
    return pl.ds(start, 8, stride=step)


def move(dst, dst_row, dst_step, src, src_row, src_step, chunks=range(ROWS // 8)):
    for chunk in chunks:
        dst[rows_at(dst_row, dst_step, chunk), :] = src[rows_at(src_row, src_step, chunk), :]


def block_copies(hbm, vmem, sems, tiles, var, inward):
    copies = []
    for tile in tiles:
        part = vmem.at[pl.ds((tile * VARS + var) * SPAN * TILE, SPAN * TILE), :]
        ends = (hbm.at[var, tile], part) if inward else (part, hbm.at[var, tile])
        copies.append(pltpu.make_async_copy(*ends, sems.at[tile * VARS + var]))
    return copies


def load_kernel(
    live, counts, ids, parent_of, x, held, msg, info, mine, other,
    counts_s, ids_s, parents, weight, fine, both, sems, small_sems,
):
    small = [
        pltpu.make_async_copy(src, dst, small_sems.at[i])
        for i, (src, dst) in enumerate(((counts, counts_s), (ids, ids_s), (parent_of, parents)))
    ]
    for copy in small:
        copy.start()
    copies = []
    for var in range(VARS):
        copies += block_copies(x, held, sems, range(LIVE_TILES), var, True)
    for copy in copies:
        copy.start()
    fill_weight(weight)
    both[...] = jnp.zeros_like(both)
    for copy in small:
        copy.wait()
    sent = counts_s[0]
    first = live[0] - sent
    lane = lanes()
    head = jnp.where(lane == SEND, sent.astype(F32), 0.0)
    for lane_id in range(SEND):
        slot = jnp.minimum(first + lane_id, LIVE - 1)
        head = jnp.where(lane == lane_id, ids_s[slot].astype(F32), head)
    msg[pl.ds(HEAD, 8), :] = head
    numbers = jnp.where(lane == LIVE_AT, live[0], 0)
    for turn in range(3):
        numbers = jnp.where(lane == COUNTS_AT + turn, counts_s[turn], numbers)
    half = mine.shape[0]
    core = lax.axis_index("bal") % PAR_DEV
    bases = []
    for slot in range(LIVE):
        mark = ids_s[slot]
        numbers = jnp.where(lane == slot, mark, numbers)
        parent = parents[mark]
        base = (parent // PAR_DEV) * FINE + jnp.bitwise_xor(parent % PAR_DEV, core) * half
        bases.append(jnp.where(slot < live[0], base, PAR_DEV * half))
    info[...] = numbers
    for copy in copies:
        copy.wait()

    groups = LIVE_TILES * VARS * SPAN // 8
    rows = held[...].reshape(groups, 8, TILE, LANES)
    pieces = []
    for side in range(4):
        at = side // 2 * 4 + side % 2
        pieces.append((rows[:, at] + rows[:, at + 2]).reshape(groups * TILE, LANES))
    pairs = jnp.concatenate(pieces, axis=1)
    high = pairs.astype(jnp.bfloat16)
    low = (pairs - high.astype(F32)).astype(jnp.bfloat16)
    w = weight[...]
    fine[...] = jnp.dot(high, w, preferred_element_type=F32) + jnp.dot(low, w, preferred_element_type=F32)
    for slot, base in enumerate(bases):
        src = (slot // TILE) * (FINE * TILE) + slot % TILE
        for start, size in ((0, 8), (8, 8), (16, 4)):
            both[pl.ds(base + start, size), :] += fine[pl.ds(src + start * TILE, size, stride=TILE), :]
    mine[...] = both[pl.ds(0, half), :]
    other[...] = both[pl.ds(half, half), :]
    for piece in range(SEND):

        @pl.when(piece < sent)
        def _(piece=piece):
            move(msg, piece * ROWS, 1, held, row_of(first + piece), TILE)


def add_kernel(mine, other, out):
    out[...] = mine[...] + other[...]


def number(ref, lane):
    return ref[HEAD, lane].astype(I32)


def head_of(ref):
    return ref[pl.ds(HEAD, 8), :]


def pick_kernel(info, held, came, last, below):
    lane = lanes()
    sent = info[0, COUNTS_AT + 1]
    kept = info[0, LIVE_AT] - info[0, COUNTS_AT]
    held_count = kept + number(came, SEND)
    marks = info[...].astype(F32)
    marks = jnp.where(lane < kept, marks, pltpu.roll(head_of(came), kept, 1))
    for msg, first, pieces in ((last, held_count - sent, sent), (below, held_count - sent - SEND, SEND)):
        head = pltpu.roll(marks, lax.rem(LANES - first, LANES), 1)
        head = jnp.where(lane == SEND, sent.astype(F32), head)
        head = jnp.where(lane == SEND + 1, info[0, COUNTS_AT + 2].astype(F32), head)
        msg[pl.ds(HEAD, 8), :] = head
        for piece in range(SEND):
            slot = first + piece
            used = jnp.logical_and(slot >= 0, piece < pieces)

            @pl.when(jnp.logical_and(used, slot < kept))
            def _(msg=msg, piece=piece, slot=slot):
                move(msg, piece * ROWS, 1, held, row_of(slot), TILE)

            @pl.when(jnp.logical_and(used, slot >= kept))
            def _(msg=msg, piece=piece, slot=slot):
                move(msg, piece * ROWS, 1, came, (slot - kept) * ROWS, 1)


def base_kernel(info, x, out, full, in_sems, out_sems):
    loads = [block_copies(x, full, in_sems, range(LIVE_TILES), var, True) for var in range(VARS)]
    for copies in loads:
        for copy in copies:
            copy.start()
    kept = info[0, LIVE_AT] - info[0, COUNTS_AT]
    sub = lax.broadcasted_iota(I32, (TILE, LANES), 0)
    full[pl.ds(LIVE_TILES * TILE_ROWS, TILE_ROWS), :] = jnp.zeros((TILE_ROWS, LANES), F32)
    stores = []
    for var in range(VARS):
        for copy in loads[var]:
            copy.wait()
        for tile in range(LIVE_TILES):
            rows = pl.ds((tile * VARS + var) * SPAN * TILE, SPAN * TILE)
            part = full[rows, :].reshape(SPAN, TILE, LANES)
            keep = (sub + tile * TILE < kept)[None]
            full[rows, :] = jnp.where(keep, part, 0.0).reshape(SPAN * TILE, LANES)
        stores += block_copies(out, full, out_sems, range(TILES), var, False)
        for copy in stores[-TILES:]:
            copy.start()
    for copy in stores:
        copy.wait()


def place_kernel(info, came, near, far, cross, base, out, new_ids, blank, sems):
    del base
    blank[...] = jnp.zeros_like(blank)
    lane = lanes()
    kept = info[0, LIVE_AT] - info[0, COUNTS_AT]
    c0 = number(came, SEND)
    c1, c2 = info[0, COUNTS_AT + 1], info[0, COUNTS_AT + 2]
    n1 = number(near, SEND)
    f2 = number(far, SEND + 1)
    x1 = number(cross, SEND)
    own = kept + c0 - c1 - jnp.maximum(c2 - n1, 0)
    from_near = jnp.maximum(n1 - c2, 0)
    from_far = jnp.maximum(f2 - x1, 0)
    from_cross = jnp.minimum(x1, f2)
    bare = jnp.minimum(own, kept)

    def copy_of(msg, row, slot, sem):
        return pltpu.make_async_copy(
            msg.at[pl.ds(row, ROWS), :].reshape(VARS, SPAN, LANES), out.at[:, slot // TILE, :, slot % TILE], sem
        )

    copies = []
    start = bare
    new = jnp.where(lane < bare, info[...].astype(F32), -1.0)
    for msg, skip, amount in (
        (came, 0, own - bare),
        (near, 0, from_near),
        (far, SEND - from_far, from_far),
        (cross, x1 - from_cross, from_cross),
    ):
        for piece in range(SEND):
            row = pl.multiple_of((skip + piece) * ROWS, 8)
            copies.append((piece < amount, msg, row, start + piece))
        moved = pltpu.roll(head_of(msg), lax.rem(start - skip + LANES, LANES), 1)
        new = jnp.where(jnp.logical_and(lane >= start, lane < start + amount), moved, new)
        start = start + amount
    copies += [(start + piece < kept, blank, 0, start + piece) for piece in range(2 * SEND)]
    for i, (used, *ends) in enumerate(copies):

        @pl.when(used)
        def _(i=i, ends=ends):
            copy_of(*ends, sems.at[i]).start()

    new_ids[...] = new[0:1, : TILE * TILES].astype(I32)
    for i, (used, *ends) in enumerate(copies):

        @pl.when(used)
        def _(i=i, ends=ends):
            copy_of(*ends, sems.at[i]).wait()


def final_kernel(mine, other, out):
    core = lax.axis_index("bal") % PAR_DEV
    out[pl.ds(core, FINE, stride=PAR_DEV), :] = mine[...]
    out[pl.ds(1 - core, FINE, stride=PAR_DEV), :] = other[...]


def call(kernel, outs, in_specs, args, out_specs, scratch=(), aliases={}):
    args = [
        pltpu.with_memory_space_constraint(arg, spec.memory_space) if spec in (VMEM, HBM) else arg
        for arg, spec in zip(args, in_specs, strict=True)
    ]
    kernel = pl.pallas_call(
        kernel,
        out_shape=outs,
        in_specs=in_specs,
        out_specs=out_specs,
        scratch_shapes=list(scratch),
        compiler_params=pltpu.CompilerParams(vmem_limit_bytes=12 << 20),
        input_output_aliases=aliases,
    )
    return kernel(*args)


def per_device(patches, patch_ids, live, counts, parent_of):
    slots = patches.shape[0]
    x = patches.transpose(1, 0, 2).reshape(VARS, TILES, TILE, SPAN, LANES)
    x = x.transpose(0, 1, 3, 2, 4).reshape(VARS, TILES, SPAN * TILE, LANES)
    counts = counts.reshape(-1)
    message = pltpu.VMEM((MSG, LANES), F32)
    dma = pltpu.SemaphoreType.DMA
    levels = lax.axis_size("level")
    half = pltpu.VMEM((levels * FINE, LANES), F32)
    held, first, info, mine, other = call(
        load_kernel,
        (pltpu.VMEM((LIVE_TILES * TILE_ROWS, LANES), F32), message, pltpu.VMEM((8, LANES), I32), half, half),
        [SMEM] + [HBM] * 4,
        (live, counts, patch_ids, parent_of, x),
        (VMEM,) * 5,
        [pltpu.SMEM(a.shape, I32) for a in (counts, patch_ids, parent_of)]
        + [
            pltpu.VMEM((4 * LANES, LANES), jnp.bfloat16),
            pltpu.VMEM((LIVE_TILES * TILE * FINE, LANES), F32),
            pltpu.VMEM((PAR_DEV * levels * FINE + 24, LANES), F32),
            dma((LIVE_TILES * VARS,)),
            dma((3,)),
        ],
    )
    came = from_partner(first, "bal", 1)
    last, below = call(pick_kernel, (message, message), [VMEM] * 3, (info, held, came), (VMEM, VMEM))
    partial = call(add_kernel, half, [VMEM, VMEM], (mine, from_partner(other, "bal", 1)), VMEM)
    far = from_partner(below, "bal", 4)
    near = from_partner(last, "bal", 2)
    cross = from_partner(last, "bal", 6)

    tiles = lax.all_to_all(partial.reshape(levels, FINE // 4, 4, LANES), "level", 0, 0, tiled=True)
    sums = jnp.sum(tiles, axis=0)
    sums = sums + from_partner(sums, "bal", 2) + from_partner(sums, "bal", 6) + from_partner(sums, "bal", 4)
    sums = sums.reshape(FINE, LANES)
    coarse = call(
        final_kernel,
        jax.ShapeDtypeStruct((FINE * PAR_DEV, LANES), F32),
        [VMEM, VMEM],
        (sums, from_partner(sums, "bal", 1)),
        VMEM,
    )
    coarse = coarse.reshape(VARS, FINE // VARS, PAR_DEV, LANES).transpose(2, 0, 1, 3).reshape(PAR_DEV, VARS, -1)

    base = call(
        base_kernel,
        jax.ShapeDtypeStruct((VARS, TILES, SPAN * TILE, LANES), F32),
        [VMEM, HBM],
        (info, x),
        HBM,
        [pltpu.VMEM((TILES * TILE_ROWS, LANES), F32), dma((LIVE_TILES * VARS,)), dma((TILES * VARS,))],
    )
    spread_out = (VARS, TILES, SPAN, TILE, LANES)
    out, new_ids = call(
        place_kernel,
        (jax.ShapeDtypeStruct(spread_out, F32), jax.ShapeDtypeStruct((1, slots), I32)),
        [VMEM, VMEM, VMEM, VMEM, VMEM, HBM],
        (info, came, near, far, cross, base.reshape(spread_out)),
        (HBM, VMEM),
        [pltpu.VMEM((ROWS, LANES), F32), dma((6 * SEND,))],
        {5: 0},
    )
    out = out.transpose(0, 1, 3, 2, 4)
    out = out.reshape(VARS, slots, SPAN * LANES).transpose(1, 0, 2)
    return (out, new_ids.reshape(slots), coarse)


def solution(mesh):
    return jax.shard_map(
        per_device,
        mesh=mesh,
        in_specs=(
            P(("level", "bal"), None, None),
            P(("level", "bal")),
            P(("level", "bal")),
            P(None, ("level", "bal")),
            P(),
        ),
        out_specs=(P(("level", "bal"), None, None), P(("level", "bal")), P("level", None, None)),
        check_vma=False,
    )
```

```python
import jax
import jax.numpy as jnp
from jax import lax
from jax.experimental import pallas as pl
from jax.experimental.pallas import tpu as pltpu
from jax.sharding import PartitionSpec as P


VARS = 5
SEND = 4
TILE = 8
TILES = 3
LIVE_TILES = 2
LIVE = 12
LANES = 128
SPAN = 32
ROWS = VARS * SPAN
TILE_ROWS = ROWS * TILE
HEAD = SEND * ROWS
MSG = HEAD + 8
FINE = 20
PAR_DEV = 2
NEAR_LEVELS = 4
F32 = jnp.float32
I32 = jnp.int32
LIVE_AT = 16
COUNTS_AT = 17

SMEM = pl.BlockSpec(memory_space=pltpu.SMEM)
VMEM = pl.BlockSpec(memory_space=pltpu.VMEM)
HBM = pl.BlockSpec(memory_space=pltpu.HBM)


def from_partner(array, axis, mask):
    return lax.ppermute(array, axis, [(i, i ^ mask) for i in range(lax.axis_size(axis))])


def place_of(level, levels):
    return (levels // NEAR_LEVELS - 1 - level // NEAR_LEVELS) * NEAR_LEVELS + level % NEAR_LEVELS


def lanes():
    return lax.broadcasted_iota(I32, (8, LANES), 1)


def row_of(slot):
    return (slot // TILE) * TILE_ROWS + slot % TILE


def fill_weight(weight):
    lane = lax.broadcasted_iota(I32, (LANES, LANES), 0)
    target = lax.broadcasted_iota(I32, (LANES, LANES), 1)
    column = (lane // 32) * 8 + (lane % 16) // 2
    for group in range(4):
        part = jnp.where(target == group * 32 + column, 0.125, 0.0)
        weight[pl.ds(group * LANES, LANES), :] = part.astype(jnp.bfloat16)


def rows_at(row, step, chunk):
    start = row + chunk * 8 * step
    if step == 1:
        return pl.ds(pl.multiple_of(start, 8), 8)
    return pl.ds(start, 8, stride=step)


def move(dst, dst_row, dst_step, src, src_row, src_step, chunks=range(ROWS // 8)):
    for chunk in chunks:
        dst[rows_at(dst_row, dst_step, chunk), :] = src[rows_at(src_row, src_step, chunk), :]


def block_copies(hbm, vmem, sems, tiles, var, inward):
    copies = []
    for tile in tiles:
        part = vmem.at[pl.ds((tile * VARS + var) * SPAN * TILE, SPAN * TILE), :]
        ends = (hbm.at[var, tile], part) if inward else (part, hbm.at[var, tile])
        copies.append(pltpu.make_async_copy(*ends, sems.at[tile * VARS + var]))
    return copies


def load_kernel(
    live, counts, ids, parent_of, x, held, info, mine, other,
    counts_s, ids_s, parents, weight, high, low, fine, both, sems, small_sems,
):
    small = [
        pltpu.make_async_copy(src, dst, small_sems.at[i])
        for i, (src, dst) in enumerate(((counts, counts_s), (ids, ids_s), (parent_of, parents)))
    ]
    for copy in small:
        copy.start()
    copies = [block_copies(x, held, sems, range(LIVE_TILES), var, True) for var in range(VARS)]
    for pair in copies:
        for copy in pair:
            copy.start()
    fill_weight(weight)
    both[...] = jnp.zeros_like(both)
    for copy in small:
        copy.wait()
    lane = lanes()
    numbers = jnp.where(lane == LIVE_AT, live[0], 0)
    for turn in range(3):
        numbers = jnp.where(lane == COUNTS_AT + turn, counts_s[turn], numbers)
    half = mine.shape[0]
    core = lax.axis_index("bal") % PAR_DEV
    bases = []
    for slot in range(LIVE):
        mark = ids_s[slot]
        numbers = jnp.where(lane == slot, mark, numbers)
        parent = parents[mark]
        base = place_of(parent // PAR_DEV, half // FINE) * FINE + jnp.bitwise_xor(parent % PAR_DEV, core) * half
        bases.append(jnp.where(slot < live[0], base, PAR_DEV * half))
    info[...] = numbers

    w = weight[...]
    part = FINE // VARS * TILE
    for var in range(VARS):
        for copy in copies[var]:
            copy.wait()
        for tile in range(LIVE_TILES):
            rows = held[pl.ds((tile * VARS + var) * SPAN * TILE, SPAN * TILE), :].reshape(-1, 8, TILE, LANES)
            to = pl.ds((tile * VARS + var) * part, part)
            for side in range(4):
                at = side // 2 * 4 + side % 2
                pairs = (rows[:, at] + rows[:, at + 2]).reshape(part, LANES)
                near = pairs.astype(jnp.bfloat16)
                high[to, pl.ds(side * LANES, LANES)] = near
                low[to, pl.ds(side * LANES, LANES)] = (pairs - near.astype(F32)).astype(jnp.bfloat16)
    fine[...] = jnp.dot(high[...], w, preferred_element_type=F32) + jnp.dot(low[...], w, preferred_element_type=F32)
    for slot, base in enumerate(bases):
        src = (slot // TILE) * (FINE * TILE) + slot % TILE
        for start, size in ((0, 8), (8, 8), (16, 4)):
            both[pl.ds(base + start, size), :] += fine[pl.ds(src + start * TILE, size, stride=TILE), :]
    mine[...] = both[pl.ds(0, half), :]
    other[...] = both[pl.ds(half, half), :]


def message_kernel(info, held, msg):
    lane = lanes()
    sent = info[0, COUNTS_AT]
    first = info[0, LIVE_AT] - sent
    head = pltpu.roll(info[...].astype(F32), lax.rem(LANES - first, LANES), 1)
    msg[pl.ds(HEAD, 8), :] = jnp.where(lane == SEND, sent.astype(F32), head)
    for piece in range(SEND):

        @pl.when(piece < sent)
        def _(piece=piece):
            move(msg, piece * ROWS, 1, held, row_of(first + piece), TILE)


def add_kernel(mine, other, out):
    out[...] = mine[...] + other[...]


def number(ref, lane):
    return ref[HEAD, lane].astype(I32)


def head_of(ref):
    return ref[pl.ds(HEAD, 8), :]


def pick_kernel(info, held, came, last, below):
    lane = lanes()
    sent = info[0, COUNTS_AT + 1]
    kept = info[0, LIVE_AT] - info[0, COUNTS_AT]
    held_count = kept + number(came, SEND)
    marks = info[...].astype(F32)
    marks = jnp.where(lane < kept, marks, pltpu.roll(head_of(came), kept, 1))
    for msg, first, pieces in ((last, held_count - sent, sent), (below, held_count - sent - SEND, SEND)):
        head = pltpu.roll(marks, lax.rem(LANES - first, LANES), 1)
        head = jnp.where(lane == SEND, sent.astype(F32), head)
        head = jnp.where(lane == SEND + 1, info[0, COUNTS_AT + 2].astype(F32), head)
        msg[pl.ds(HEAD, 8), :] = head
        for piece in range(SEND):
            slot = first + piece
            used = jnp.logical_and(slot >= 0, piece < pieces)

            @pl.when(jnp.logical_and(used, slot < kept))
            def _(msg=msg, piece=piece, slot=slot):
                move(msg, piece * ROWS, 1, held, row_of(slot), TILE)

            @pl.when(jnp.logical_and(used, slot >= kept))
            def _(msg=msg, piece=piece, slot=slot):
                move(msg, piece * ROWS, 1, came, (slot - kept) * ROWS, 1)


def base_kernel(info, x, out, full, in_sems, out_sems):
    loads = [block_copies(x, full, in_sems, range(LIVE_TILES), var, True) for var in range(VARS)]
    for copies in loads:
        for copy in copies:
            copy.start()
    kept = info[0, LIVE_AT] - info[0, COUNTS_AT]
    sub = lax.broadcasted_iota(I32, (TILE, LANES), 0)
    full[pl.ds(LIVE_TILES * TILE_ROWS, TILE_ROWS), :] = jnp.zeros((TILE_ROWS, LANES), F32)
    stores = []
    for var in range(VARS):
        for copy in loads[var]:
            copy.wait()
        for tile in range(LIVE_TILES):
            rows = pl.ds((tile * VARS + var) * SPAN * TILE, SPAN * TILE)
            part = full[rows, :].reshape(SPAN, TILE, LANES)
            keep = (sub + tile * TILE < kept)[None]
            full[rows, :] = jnp.where(keep, part, 0.0).reshape(SPAN * TILE, LANES)
        stores += block_copies(out, full, out_sems, range(TILES), var, False)
        for copy in stores[-TILES:]:
            copy.start()
    for copy in stores:
        copy.wait()


def place_kernel(info, came, near, far, cross, base, out, new_ids, blank, sems):
    del base
    blank[...] = jnp.zeros_like(blank)
    lane = lanes()
    kept = info[0, LIVE_AT] - info[0, COUNTS_AT]
    c0 = number(came, SEND)
    c1, c2 = info[0, COUNTS_AT + 1], info[0, COUNTS_AT + 2]
    n1 = number(near, SEND)
    f2 = number(far, SEND + 1)
    x1 = number(cross, SEND)
    own = kept + c0 - c1 - jnp.maximum(c2 - n1, 0)
    from_near = jnp.maximum(n1 - c2, 0)
    from_far = jnp.maximum(f2 - x1, 0)
    from_cross = jnp.minimum(x1, f2)
    bare = jnp.minimum(own, kept)

    def copy_of(msg, row, slot, sem):
        return pltpu.make_async_copy(
            msg.at[pl.ds(row, ROWS), :].reshape(VARS, SPAN, LANES), out.at[:, slot // TILE, :, slot % TILE], sem
        )

    copies = []
    start = bare
    new = jnp.where(lane < bare, info[...].astype(F32), -1.0)
    for msg, skip, amount in (
        (came, 0, own - bare),
        (near, 0, from_near),
        (far, SEND - from_far, from_far),
        (cross, x1 - from_cross, from_cross),
    ):
        for piece in range(SEND):
            row = pl.multiple_of((skip + piece) * ROWS, 8)
            copies.append((piece < amount, msg, row, start + piece))
        moved = pltpu.roll(head_of(msg), lax.rem(start - skip + LANES, LANES), 1)
        new = jnp.where(jnp.logical_and(lane >= start, lane < start + amount), moved, new)
        start = start + amount
    copies += [(start + piece < kept, blank, 0, start + piece) for piece in range(2 * SEND)]
    for i, (used, *ends) in enumerate(copies):

        @pl.when(used)
        def _(i=i, ends=ends):
            copy_of(*ends, sems.at[i]).start()

    new_ids[...] = new[0:1, : TILE * TILES].astype(I32)
    for i, (used, *ends) in enumerate(copies):

        @pl.when(used)
        def _(i=i, ends=ends):
            copy_of(*ends, sems.at[i]).wait()


def final_kernel(mine, other, out):
    core = lax.axis_index("bal") % PAR_DEV
    out[pl.ds(core, FINE, stride=PAR_DEV), :] = mine[...]
    out[pl.ds(1 - core, FINE, stride=PAR_DEV), :] = other[...]


def call(kernel, outs, in_specs, args, out_specs, scratch=(), aliases={}):
    args = [
        pltpu.with_memory_space_constraint(arg, spec.memory_space) if spec in (VMEM, HBM) else arg
        for arg, spec in zip(args, in_specs, strict=True)
    ]
    kernel = pl.pallas_call(
        kernel,
        out_shape=outs,
        in_specs=in_specs,
        out_specs=out_specs,
        scratch_shapes=list(scratch),
        compiler_params=pltpu.CompilerParams(vmem_limit_bytes=12 << 20),
        input_output_aliases=aliases,
    )
    return kernel(*args)


def per_device(patches, patch_ids, live, counts, parent_of):
    slots = patches.shape[0]
    x = patches.transpose(1, 0, 2).reshape(VARS, TILES, TILE, SPAN, LANES)
    x = x.transpose(0, 1, 3, 2, 4).reshape(VARS, TILES, SPAN * TILE, LANES)
    counts = counts.reshape(-1)
    message = pltpu.VMEM((MSG, LANES), F32)
    dma = pltpu.SemaphoreType.DMA
    levels = lax.axis_size("level")
    half = pltpu.VMEM((levels * FINE, LANES), F32)
    held, info, mine, other = call(
        load_kernel,
        (pltpu.VMEM((LIVE_TILES * TILE_ROWS, LANES), F32), pltpu.VMEM((8, LANES), I32), half, half),
        [SMEM] + [HBM] * 4,
        (live, counts, patch_ids, parent_of, x),
        (VMEM,) * 4,
        [pltpu.SMEM(a.shape, I32) for a in (counts, patch_ids, parent_of)]
        + [
            pltpu.VMEM((4 * LANES, LANES), jnp.bfloat16),
            pltpu.VMEM((LIVE_TILES * TILE * FINE, 4 * LANES), jnp.bfloat16),
            pltpu.VMEM((LIVE_TILES * TILE * FINE, 4 * LANES), jnp.bfloat16),
            pltpu.VMEM((LIVE_TILES * TILE * FINE, LANES), F32),
            pltpu.VMEM((PAR_DEV * levels * FINE + 24, LANES), F32),
            dma((LIVE_TILES * VARS,)),
            dma((3,)),
        ],
    )
    first = call(message_kernel, message, [VMEM, VMEM], (info, held), VMEM)
    came = from_partner(first, "bal", 1)
    last, below = call(pick_kernel, (message, message), [VMEM] * 3, (info, held, came), (VMEM, VMEM))
    partial = call(add_kernel, half, [VMEM, VMEM], (mine, from_partner(other, "bal", 1)), VMEM)
    far = from_partner(below, "bal", 4)
    near = from_partner(last, "bal", 2)
    cross = from_partner(last, "bal", 6)

    order = [place_of(level, levels) for level in range(levels)]
    tiles = lax.all_to_all(
        partial.reshape(levels, FINE // 4, 4, LANES), "level", 0, 0, axis_index_groups=[order], tiled=True
    )
    sums = jnp.sum(tiles, axis=0)
    sums = sums + from_partner(sums, "bal", 2) + from_partner(sums, "bal", 6) + from_partner(sums, "bal", 4)
    sums = sums.reshape(FINE, LANES)
    coarse = call(
        final_kernel,
        jax.ShapeDtypeStruct((FINE * PAR_DEV, LANES), F32),
        [VMEM, VMEM],
        (sums, from_partner(sums, "bal", 1)),
        VMEM,
    )
    coarse = coarse.reshape(VARS, FINE // VARS, PAR_DEV, LANES).transpose(2, 0, 1, 3).reshape(PAR_DEV, VARS, -1)

    base = call(
        base_kernel,
        jax.ShapeDtypeStruct((VARS, TILES, SPAN * TILE, LANES), F32),
        [VMEM, HBM],
        (info, x),
        HBM,
        [pltpu.VMEM((TILES * TILE_ROWS, LANES), F32), dma((LIVE_TILES * VARS,)), dma((TILES * VARS,))],
    )
    spread_out = (VARS, TILES, SPAN, TILE, LANES)
    out, new_ids = call(
        place_kernel,
        (jax.ShapeDtypeStruct(spread_out, F32), jax.ShapeDtypeStruct((1, slots), I32)),
        [VMEM, VMEM, VMEM, VMEM, VMEM, HBM],
        (info, came, near, far, cross, base.reshape(spread_out)),
        (HBM, VMEM),
        [pltpu.VMEM((ROWS, LANES), F32), dma((6 * SEND,))],
        {5: 0},
    )
    out = out.transpose(0, 1, 3, 2, 4)
    out = out.reshape(VARS, slots, SPAN * LANES).transpose(1, 0, 2)
    return (out, new_ids.reshape(slots), coarse)


def solution(mesh):
    return jax.shard_map(
        per_device,
        mesh=mesh,
        in_specs=(
            P(("level", "bal"), None, None),
            P(("level", "bal")),
            P(("level", "bal")),
            P(None, ("level", "bal")),
            P(),
        ),
        out_specs=(P(("level", "bal"), None, None), P(("level", "bal")), P("level", None, None)),
        check_vma=False,
    )
```
